32 devices in a mesh: dp: 4 (over y, x), feature: 8 (over z, core).
Axes of the slice: x: 2, y: 2, z: 4, core: 2. Of those that a mesh axis runs over, the one named last changes fastest.
Arguments:
- tokens_in: bfloat16 [2048, 16384], P('dp', 'feature'), may hold values from -6 to 6
- key_grad: bfloat16 [2048, 1024], P('dp'), may hold values from -0.119628906 to 0.119628906
- eig_in: float32 [16384, 16384], P('feature', 'dp'), may hold values from -0.0625 to 0.0625
- eig_out: float32 [1024, 1024], replicated, may hold values from -0.1875 to 0.1875
- eigenvalues: float32 [16384, 1024], P(('dp', 'feature')), may hold values from 0.1 to 10
Outputs:
- update: float32 [16384, 1024], P(('feature', 'dp'))
The draws below stay inside these ranges and needn't reach their ends.
All inputs are finite; a program needn't handle non-finite values.
Results may differ from the reference program's by a relative error of at most 0.0003.
Values sent between devices are 32-bit elements; how exact they have to be, the bound alone decides.
No kernel may reach another device: no remote copies, remote signals or barrier semaphores. Data moves between devices by JAX's collectives and lax.ppermute only.
A program may use at most 128 MiB of HBM per device.

```python
import math
import jax
import jax.numpy as jnp
from jax import lax

D = 16384
KV = 1024
TOKENS = 2048


def spiked(array, own_key, source, target, shards_of, factor):
    def block_of(position):
        return (jnp.arange(array.shape[position]) // (array.shape[position] // shards_of)).reshape((-1,) + (1,) * (array.ndim - 1 - position))

    one_side = jax.random.permutation(own_key, shards_of)[block_of(target)]
    other_side = (block_of(target) + shards_of // 2) % shards_of
    return jnp.where((block_of(source) == one_side) | (block_of(source) == other_side), factor * array, array)


def block_scale(key, extent, cuts, low, largest):
    factor_of, own = 1.0, jax.random.fold_in(key, 6)
    for axis_at, shards_of in cuts:
        draws = jnp.exp(jax.random.uniform(jax.random.fold_in(own, axis_at), (shards_of,), jnp.float32, low / len(cuts), largest / len(cuts)))
        factor_of = factor_of * jnp.repeat(draws, extent[axis_at] // shards_of).reshape([-1 if axis == axis_at else 1 for axis in range(len(extent))])
    return factor_of


def gaussian(own_key, dims, spread, reach, shards=(), held_as=jnp.bfloat16):
    result = spread * jax.random.normal(own_key, dims, jnp.float32)
    if shards:
        result = result * block_scale(own_key, dims, shards, -0.22, 0.18)
    return jnp.clip(result, -reach, reach).astype(held_as)


def gaussian_with(stream_key, extent, width, limit, pieces, heavy, kind=jnp.bfloat16):
    values = width * jax.random.normal(stream_key, extent, jnp.float32)
    if pieces:
        values = values * block_scale(stream_key, extent, pieces, -0.22, 0.18)
    return jnp.clip(spiked(values, jax.random.fold_in(stream_key, 3), *heavy), -limit, limit).astype(kind)


def setup_inputs(seed: int = 0) -> dict:
    seeds = jax.random.split(jax.random.key(seed), 6)
    tokens_in = gaussian(seeds[0], (TOKENS, D), 1.0, 6.0, ((0, 4), (1, 8)))
    key_grad = gaussian(seeds[1], (TOKENS, KV), 0.02, 0.119628906, ((0, 4),))
    eig_in = gaussian_with(seeds[2], (D, D), D ** -0.5, 0.0625, ((0, 8), (1, 4)), (0, 1, 8, 2.0), jnp.float32)
    eig_out = gaussian(seeds[3], (KV, KV), KV ** -0.5, 0.1875, (), jnp.float32)
    eigenvalues = jnp.clip(jnp.exp(math.log(10.0) - 4.6051702 * jax.random.uniform(seeds[4], (D, KV), jnp.float32) ** block_scale(seeds[4], (D, KV), ((0, 32),), -0.2, 0.2)), 0.1, 10.0)
    return dict(tokens_in=tokens_in, key_grad=key_grad, eig_in=eig_in, eig_out=eig_out, eigenvalues=eigenvalues)


damping = 0.1


def reference(tokens_in, key_grad, eig_in, eig_out, eigenvalues):
    grad = lax.dot_general(tokens_in, key_grad, (((0,), (0,)), ((), ())), preferred_element_type=jnp.float32)
    rotated = lax.dot_general(eig_in, grad, (((0,), (0,)), ((), ())), precision=lax.Precision.HIGHEST, preferred_element_type=jnp.float32)
    scaled = jnp.dot(rotated, eig_out, precision=lax.Precision.HIGHEST, preferred_element_type=jnp.float32)
    damped = scaled / (eigenvalues + damping)
    back = lax.dot_general(damped, eig_out, (((1,), (1,)), ((), ())), precision=lax.Precision.HIGHEST, preferred_element_type=jnp.float32)
    return jnp.dot(eig_in, back, precision=lax.Precision.HIGHEST, preferred_element_type=jnp.float32)
```

```python
import functools

import jax
import jax.numpy as jnp
from jax import lax
from jax.experimental import pallas as pl
from jax.experimental.pallas import tpu as pltpu
from jax.sharding import PartitionSpec as P

damping = 0.1
shares = (2, 2, 2, 2)
cores = 2
lanes = 128


def halves_of(value):
    high = lax.reduce_precision(value, 8, 7)
    return high.astype(jnp.bfloat16), (value - high).astype(jnp.bfloat16)


def halves_in_kernel(value):
    high = value.astype(jnp.bfloat16)
    return high, (value - high.astype(jnp.float32)).astype(jnp.bfloat16)


def dot(left, right):
    return jnp.dot(left, right, preferred_element_type=jnp.float32)


def exact_left(left, right, dims):
    high, low = halves_of(right)
    parts = [
        lax.dot_general(part, left, (dims, ((), ())), preferred_element_type=jnp.float32)
        for part in (high, low)
    ]
    return parts[0] + parts[1]


def product(left, right, dims):
    return lax.dot_general(
        left, right, dims, precision=lax.Precision.HIGH, preferred_element_type=jnp.float32
    )


def columns_of(basis, table):
    height, width = basis.shape
    return jnp.take(basis.reshape(height, cores * table.shape[0], -1), table, axis=1)


def rotate_kernel(table, grad, basis, out, stacked):
    rows = grad.shape[0]

    @pl.when(pl.program_id(0) == 0)
    def _():
        high, low = halves_in_kernel(grad[...])
        stacked[:rows] = high
        stacked[rows:] = low

    high, low = halves_in_kernel(basis[...])
    both = dot(stacked[...], high)
    out[0] = both[:rows] + both[rows:] + dot(stacked[:rows], low)


def rotate(table, grad, basis):
    rows, depth = grad.shape
    slots = table.shape[0]
    block = basis.shape[1] // (cores * slots)
    if block % lanes:
        out = product(grad, columns_of(basis, table), (((1,), (0,)), ((), ())))
        return out.transpose(1, 0, 2)
    return pl.pallas_call(
        rotate_kernel,
        grid_spec=pltpu.PrefetchScalarGridSpec(
            num_scalar_prefetch=1,
            grid=(slots,),
            in_specs=[
                pl.BlockSpec((rows, depth), lambda at, ref: (0, 0)),
                pl.BlockSpec((depth, block), lambda at, ref: (0, ref[at])),
            ],
            out_specs=pl.BlockSpec((1, rows, block), lambda at, ref: (at, 0, 0)),
            scratch_shapes=[pltpu.VMEM((2 * rows, depth), jnp.bfloat16)],
        ),
        out_shape=jax.ShapeDtypeStruct((slots, rows, block), jnp.float32),
        compiler_params=pltpu.CompilerParams(
            dimension_semantics=("arbitrary",), vmem_limit_bytes=32 * 2**20
        ),
        cost_estimate=pl.CostEstimate(
            flops=6 * rows * basis.size // cores, transcendentals=0, bytes_accessed=4 * basis.size // cores
        ),
        name="rotate",
    )(table, grad, basis)


def restore_kernel(table, rows, basis, *refs):
    out = refs[-1]
    columns = out.shape[1]

    @pl.when(pl.program_id(0) == 0)
    def _():
        out[...] = refs[0][...] if len(refs) == 2 else jnp.zeros_like(out)

    high, low = halves_in_kernel(basis[...])
    rows_high, rows_low = halves_in_kernel(rows[0])
    both = dot(high, jnp.concatenate([rows_high, rows_low], axis=1))
    out[...] += both[:, :columns] + both[:, columns:] + dot(low, rows_high)


def restore(table, rows, basis, so_far=None):
    slots, block, columns = rows.shape
    height = basis.shape[0]
    if block % lanes:
        out = product(columns_of(basis, table), rows, (((1, 2), (0, 1)), ((), ())))
        return out if so_far is None else so_far + out
    whole = pl.BlockSpec((height, columns), lambda at, ref: (0, 0))
    more = [] if so_far is None else [so_far]
    return pl.pallas_call(
        restore_kernel,
        grid_spec=pltpu.PrefetchScalarGridSpec(
            num_scalar_prefetch=1,
            grid=(slots,),
            in_specs=[
                pl.BlockSpec((1, block, columns), lambda at, ref: (at, 0, 0)),
                pl.BlockSpec((height, block), lambda at, ref: (0, ref[at])),
            ] + [whole] * len(more),
            out_specs=whole,
        ),
        out_shape=jax.ShapeDtypeStruct((height, columns), jnp.float32),
        compiler_params=pltpu.CompilerParams(
            dimension_semantics=("arbitrary",), vmem_limit_bytes=40 * 2**20
        ),
        cost_estimate=pl.CostEstimate(
            flops=6 * columns * basis.size // cores, transcendentals=0, bytes_accessed=4 * basis.size // cores
        ),
        name="restore",
    )(table, rows, basis, *more)


def damp_kernel(block, low, high, values, out):
    out[...] = (block[...] + low[...] + high[...]).T / (values[...] + damping)


def damp(block, low, high, values, start):
    columns, rows = block.shape
    whole = pl.BlockSpec((columns, rows), lambda step: (0, 0))
    return pl.pallas_call(
        damp_kernel,
        grid=(1,),
        in_specs=[whole] * 3 + [pl.BlockSpec((rows, columns), lambda step: (0, start // columns))],
        out_specs=pl.BlockSpec((rows, columns), lambda step: (0, 0)),
        out_shape=jax.ShapeDtypeStruct((rows, columns), jnp.float32),
        compiler_params=pltpu.CompilerParams(vmem_limit_bytes=16 * 2**20),
        name="damp",
    )(block, low, high, values)


def other_core(value, slots):
    pairs = [(at, at ^ 1) for at in range(cores * slots)]
    return lax.ppermute(value, "feature", pairs)


def up(value, slots, low, high):
    pairs = [
        (cores * at + core, cores * (at + 1) + core) for at in range(low, high) for core in range(cores)
    ]
    return lax.ppermute(value, "feature", pairs)


def down(value, slots, low, high):
    pairs = [
        (cores * (at + 1) + core, cores * at + core) for at in range(low, high) for core in range(cores)
    ]
    return lax.ppermute(value, "feature", pairs)


def fence(state):
    keys = list(state)
    state.update(zip(keys, lax.optimization_barrier([state[key] for key in keys])))


def spans_of(width):
    unit, start, spans = width // sum(shares), 0, {}
    for at in sorted(range(len(shares)), key=lambda at: -shares[at]):
        spans[at] = slice(start, start + shares[at] * unit)
        start = spans[at].stop
    return spans


def solution(mesh):
    slots = mesh.shape["feature"] // cores
    chunks = len(shares)

    def on_device(tokens_in, key_grad, eig_in, eig_out, eigenvalues):
        place = lax.axis_index("feature")
        places = (place // cores + jnp.arange(slots, dtype=jnp.int32)) % slots * cores
        own_table = (places + place % cores).astype(jnp.int32)
        peer_table = (places + 1 - place % cores).astype(jnp.int32)
        spans = spans_of(eig_out.shape[0])
        keys = exact_left(key_grad, eig_out, ((0,), (1,)))
        part = lambda at: exact_left(tokens_in, keys[spans[at]], ((1,), (0,)))

        def collect(rows):
            return lax.psum_scatter(rows, "dp", scatter_dimension=0, tiled=True)

        def back(rows, at):
            return product(rows, eig_out[:, spans[at]], (((1,), (1,)), ((), ())))

        def forward(state, phase):
            if phase == 0:
                if "peer" in state:
                    state["got"] = other_core(state.pop("peer"), slots)
                state["own"] = rotate(own_table, state.pop("grad"), eig_in)
                return
            at, to = slots - phase, phase
            if phase == 1:
                got, own = state.pop("got"), state.pop("own")
                for slot in range(slots):
                    state[slot] = own[slot] + got[slot]
            else:
                state[at] = state[at] + state.pop("low")
                state[to] = state[to] + state.pop("high")
            state["low"] = up(state[at], slots, 0, phase)
            state["high"] = down(state[to], slots, slots - 1 - phase, slots - 1)
            if at <= to:
                for slot in {at, to}:
                    state.pop(slot)

        def backward(state, phase):
            if phase < slots - 1:
                low = state["low", phase - 1] if phase else state["block"]
                high = state["high", phase - 1] if phase else state["block"]
                state["low", phase] = up(low, slots, phase, slots - 1)
                state["high", phase] = down(high, slots, 0, slots - 1 - phase)
            else:
                blocks = [state.pop("block")] + [
                    state.pop(("high", at - 1)) + state.pop(("low", slots - at - 1)) for at in range(1, slots)
                ]
                blocks = jnp.stack(blocks)
                state["peer"] = other_core(blocks, slots)
                state["rows"] = restore(own_table, blocks, eig_in)

        def late(state, phase):
            if phase == 1:
                state["rows"] = restore(peer_table, state.pop("peer"), eig_in, state["rows"])

        def early(state, phase, turn):
            first = slots - 2 if turn else slots - 1
            if phase == first:
                state["grad"] = grads[turn + 1]
                state["peer"] = rotate(peer_table, state["grad"], eig_in)
                if turn + 2 < chunks:
                    state["part"] = part(turn + 2)
            elif phase == first + 1:
                state["got"] = other_core(state.pop("peer"), slots)

        grads = [lax.psum(part(0), "dp")]
        after, grads[0] = lax.optimization_barrier((part(1), grads[0]))
        grads.append(lax.psum(after, "dp"))
        ahead = {"grad": grads[0], "peer": rotate(peer_table, grads[0], eig_in)}
        ahead["peer"], ahead["grad"] = lax.optimization_barrier((ahead["peer"], ahead["grad"]))
        behind, last, ours = None, None, []
        for turn in range(chunks + 1):
            coming = {} if turn + 1 < chunks else None
            for phase in range(slots):
                if ahead is not None:
                    forward(ahead, phase)
                if behind is not None:
                    backward(behind, phase)
                if last is not None:
                    late(last, phase)
                if coming is not None:
                    early(coming, phase, turn)
                state, stages = {}, (ahead, behind, last, coming)
                for which, stage in enumerate(stages):
                    if stage is not None:
                        state.update({(which, key): value for key, value in stage.items()})
                if phase == slots - 1 and ours:
                    state["ours"] = ours[-1]
                fence(state)
                if "ours" in state:
                    ours[-1] = state["ours"]
                for which, stage in enumerate(stages):
                    if stage is not None:
                        stage.update({key: state[which, key] for key in stage})
                if coming is not None and "part" in coming:
                    grads.append(lax.psum(coming.pop("part"), "dp"))
                if last is not None and phase == 1:
                    ours.append(collect(last["rows"]))
                    last = None
            last, behind = behind, None
            if ahead is not None:
                start = spans[turn].start
                behind = {"block": damp(ahead[0], ahead["low"], ahead["high"], eigenvalues, start)}
            ahead = coming
        late(last, 1)
        ours.append(collect(last["rows"]))
        return functools.reduce(jnp.add, [back(rows, at) for at, rows in enumerate(ours)])

    in_specs = (
        P("dp", "feature"),
        P("dp", None),
        P("feature", "dp"),
        P(),
        P(("dp", "feature"), None),
    )
    return jax.shard_map(
        on_device, mesh=mesh, in_specs=in_specs, out_specs=P(("feature", "dp"), None),
        check_vma=False,
    )
```
